32 devices in a mesh: pair: 2 (over y), dp: 8 (over z, x), ep: 2 (over core).
Axes of the slice: x: 2, y: 2, z: 4, core: 2. Of those that a mesh axis runs over, the one named last changes fastest.
Arguments:
- activations: bfloat16 [12288, 1024], P(('pair', 'dp'), 'ep'), parts along dimension 1, may hold values from -6 to 6
- cotangents: bfloat16 [12288, 4096], P(('pair', 'dp'), 'ep'), parts along dimension 1, may hold values from -0.875 to 0.875
Outputs:
- averaged_grad: bfloat16 [512, 4096], P('pair', 'ep'), parts along dimension 1
The draws below stay inside these ranges and needn't reach their ends.
There are 2 independent parts, one for each index of `ep`. The reference program is written for one: setup_inputs(seed, part) draws one part's arguments, and reference() takes and returns one part's arrays. A program takes and returns all parts, laid end to end along the dimension named above; each array names one. Nothing has to cross between parts.
All inputs are finite; a program needn't handle non-finite values.
Results may differ from the reference program's by a relative error of at most 0.001.
Values may be sent and summed in bfloat16 or wider, within the bound.
A program may use at most 64 MiB of HBM per device.

```python
import jax
import jax.numpy as jnp

FF = 2048
ROWS = 512
TOK_DEV = 768
REPLICAS = 16
TOKENS = 12288
N_PAIR = 2
N_DP = 8


def raised(drawn, stream_key, source, target, parts, factor):
    def block_of(position):
        return (jnp.arange(drawn.shape[position]) // (drawn.shape[position] // parts)).reshape((-1,) + (1,) * (drawn.ndim - 1 - position))

    near = jax.random.permutation(stream_key, parts)[block_of(target)]
    second = (block_of(target) + parts // 2) % parts
    return jnp.where((block_of(source) == near) | (block_of(source) == second), factor * drawn, drawn)


def steps_of(own_key, extent, cuts, least, largest):
    def one(position, parts):
        draws = jax.random.uniform(jax.random.fold_in(jax.random.fold_in(own_key, 6), position), (parts,), jnp.float32, least / len(cuts), largest / len(cuts))
        return jnp.repeat(jnp.exp(draws), extent[position] // parts).reshape((-1,) + (1,) * (len(extent) - position - 1))

    factor_of = one(*cuts[0])
    for cut in cuts[1:]:
        factor_of = factor_of * one(*cut)
    return factor_of


def scatter_about(key, shape, scale, bound, cuts=(), held_as=jnp.bfloat16):
    entries = jax.random.normal(key, shape, jnp.float32) * scale
    if len(cuts) > 0:
        entries = steps_of(key, shape, cuts, -0.22, 0.18) * entries
    return jnp.clip(entries, min=-bound, max=bound).astype(held_as)


def gaussian_with(own_key, dims, scale, limit, cuts, heavy, held_as=jnp.bfloat16):
    drawn = scale * jax.random.normal(own_key, dims, jnp.float32)
    if cuts:
        drawn = drawn * steps_of(own_key, dims, cuts, -0.22, 0.18)
    return jnp.clip(raised(drawn, jax.random.fold_in(own_key, 3), *heavy), -limit, limit).astype(held_as)


def setup_inputs(seed: int = 0, part: int = 0) -> dict:
    keys = jax.random.split(jax.random.key(seed), 3)
    part_keys = jax.random.split(jax.random.fold_in(keys[2], part), 3)
    return {
        "activations": gaussian_with(part_keys[0], (TOKENS, ROWS), 1.0, 6.0, ((0, 16),), (0, 1, 16, 2.0)),
        "cotangents": scatter_about(part_keys[1], (TOKENS, FF), (max(1, TOK_DEV // (N_PAIR * N_DP))) ** -0.5, 0.875, ((0, 16),)),
    }


def reference(activations, cotangents):
    grad_sum = jnp.dot(activations.T, cotangents, preferred_element_type=jnp.float32)
    return (grad_sum / REPLICAS).astype(jnp.bfloat16)
```

```python
import functools
import math

import jax
import jax.numpy as jnp
from jax import lax
from jax.experimental import pallas as pl
from jax.experimental.pallas import tpu as pltpu
from jax.sharding import PartitionSpec as P

LANES = 128
SPLIT = 2
AHEAD = 3
CROSS = 2
LAG = (4, 7, 10)
POWER = 11
LARGEST_PRODUCT = 16 * 1.75


def scale_and_offset(terms):
    scale = 2.0 ** math.floor(126 / POWER - math.log2(terms * LARGEST_PRODUCT))
    return scale, 2.0 ** (-124 / POWER)


def encode(x, terms):
    scale, offset = scale_and_offset(terms)
    a = x * scale + jnp.where(x < 0, -offset, offset)
    a2 = a * a
    a4 = a2 * a2
    return (a4 * a4 * (a2 * a)).astype(jnp.bfloat16)


def decode(f, terms):
    scale, offset = scale_and_offset(terms)
    f = f.astype(jnp.float32)
    a = (jnp.exp2(jnp.log2(jnp.abs(f)) * (1 / POWER)) - offset) * (1 / scale)
    return jnp.where(f < 0, -a, a)


def kernel(np_, nx, nz, nc, ns, act_hbm, cot_hbm, out_ref, act_ref, cot_ref, act_t, part, enc, f1, f2, zr,
           s1, r1, s2, r2, sz, rz, sg, rg, sx, rx, load):
    p = lax.axis_index("pair")
    dp = lax.axis_index("dp")
    z, x = dp // nx, dp % nx
    rs = part.shape[-2]
    chunks = nc * ns
    rows_p = nz * ns * rs
    cols_x = nc * LANES
    terms = act_ref.shape[0]

    def other(i, q, n):
        return lax.rem(i + q, n)

    def to_pair(q):
        return {"pair": other(p, q, np_)}

    def to_x(q):
        return {"dp": z * nx + other(x, q, nx)}

    def to_z(q):
        return {"dp": other(z, q, nz) * nx + x}

    def crossed(k):
        return lax.rem(k, CROSS) == CROSS - 1

    def remote(src, dst, ssem, rsem, peer):
        return pltpu.make_async_remote_copy(
            src_ref=src, dst_ref=dst, send_sem=ssem, recv_sem=rsem,
            device_id=peer, device_id_type=pl.DeviceIdType.MESH)

    def first_a(k, q):
        return remote(enc.at[k, other(p, q, np_)], f1.at[k, pl.ds(p * nx, nx)],
                      s1.at[k, q], r1.at[k, p], to_pair(q))

    def first_b(k, q):
        return remote(enc.at[k, :, other(x, q, nx)], f1.at[k, pl.ds(x * np_, np_)],
                      s1.at[k, q], r1.at[k, x], to_x(q))

    def second_a(k, q):
        return remote(enc.at[k, p, other(x, q, nx)], f2.at[k, x], s2.at[k, q], r2.at[k, x], to_x(q))

    def second_b(k, q):
        return remote(enc.at[k, other(p, q, np_), x], f2.at[k, p], s2.at[k, q], r2.at[k, p], to_pair(q))

    def along_z(k, q):
        return remote(enc.at[k, p, x, other(z, q, nz)], zr.at[k, z], sz.at[k, q], rz.at[k, z], to_z(q))

    def piece(k, zi, xi):
        c, s = k // ns, lax.rem(k, ns)
        row = pl.multiple_of((zi * ns + s) * rs, rs)
        col = pl.multiple_of(xi * cols_x + c * LANES, LANES)
        return out_ref.at[pl.ds(row, rs), pl.ds(col, LANES)]

    def gather_z(k, q):
        here = piece(k, z, x)
        return remote(here, here, sg.at[k, q], rg.at[k, z], to_z(q))

    def gather_x(k, zo, q):
        zi = other(z, zo, nz)
        here = piece(k, zi, x)
        return remote(here, here, sx.at[k, zi, q], rx.at[k, zi, x], to_x(q))

    def arrived(dst, ssem, rsem):
        remote(dst, dst, ssem, rsem, to_pair(1)).wait_recv()

    def start_first(k):
        @pl.when(crossed(k))
        def _():
            for q in range(1, nx):
                o = other(x, q, nx)
                enc[k, :, o] = encode(part[k, :, o], terms)
                first_b(k, q).start()

        @pl.when(jnp.logical_not(crossed(k)))
        def _():
            for q in range(1, np_):
                o = other(p, q, np_)
                enc[k, o] = encode(part[k, o], terms)
                first_a(k, q).start()

    def stage2(k):
        @pl.when(jnp.logical_not(crossed(k)))
        def _():
            for q in range(1, np_):
                o = other(p, q, np_)
                arrived(f1.at[k, pl.ds(o * nx, nx)], s1.at[k, q], r1.at[k, o])
                for i in range(nx):
                    part[k, p, i] += decode(f1[k, o * nx + i], terms)
            for q in range(1, nx):
                o = other(x, q, nx)
                enc[k, p, o] = encode(part[k, p, o], np_ * terms)
                second_a(k, q).start()

        @pl.when(crossed(k))
        def _():
            for q in range(1, nx):
                o = other(x, q, nx)
                arrived(f1.at[k, pl.ds(o * np_, np_)], s1.at[k, q], r1.at[k, o])
                for i in range(np_):
                    part[k, i, x] += decode(f1[k, o * np_ + i], terms)
            for q in range(1, np_):
                o = other(p, q, np_)
                enc[k, o, x] = encode(part[k, o, x], nx * terms)
                second_b(k, q).start()

    def stage3(k):
        @pl.when(jnp.logical_not(crossed(k)))
        def _():
            for q in range(1, nx):
                o = other(x, q, nx)
                arrived(f2.at[k, o], s2.at[k, q], r2.at[k, o])
                part[k, p, x] += decode(f2[k, o], np_ * terms)

        @pl.when(crossed(k))
        def _():
            for q in range(1, np_):
                o = other(p, q, np_)
                arrived(f2.at[k, o], s2.at[k, q], r2.at[k, o])
                part[k, p, x] += decode(f2[k, o], nx * terms)

        for q in range(1, nz):
            o = other(z, q, nz)
            enc[k, p, x, o] = encode(part[k, p, x, o], np_ * nx * terms)
            along_z(k, q).start()

    def stage4(k):
        total = part[k, p, x, z]
        for q in range(1, nz):
            o = other(z, q, nz)
            arrived(zr.at[k, o], sz.at[k, q], rz.at[k, o])
            total = total + decode(zr[k, o], np_ * nx * terms)
        replicas = np_ * nx * nz
        piece(k, z, x)[...] = (total / replicas).astype(out_ref.dtype)
        for q in range(1, nz):
            gather_z(k, q).start()
        for q in range(1, nx):
            gather_x(k, 0, q).start()

    def stage5(k):
        for zo in range(1, nz):
            o = other(z, zo, nz)
            arrived(piece(k, o, x), sg.at[k, zo], rg.at[k, o])
            for q in range(1, nx):
                gather_x(k, zo, q).start()

    def stage6(k):
        for zi in range(nz):
            for q in range(1, nx):
                o = other(x, q, nx)
                arrived(piece(k, zi, o), sx.at[k, zi, q], rx.at[k, zi, o])

    def finish(k):
        @pl.when(jnp.logical_not(crossed(k)))
        def _():
            for q in range(1, np_):
                first_a(k, q).wait_send()
            for q in range(1, nx):
                second_a(k, q).wait_send()

        @pl.when(crossed(k))
        def _():
            for q in range(1, nx):
                first_b(k, q).wait_send()
            for q in range(1, np_):
                second_b(k, q).wait_send()

        for q in range(1, nz):
            along_z(k, q).wait_send()
            gather_z(k, q).wait_send()
        for zo in range(nz):
            for q in range(1, nx):
                gather_x(k, zo, q).wait_send()

    barrier = pltpu.get_barrier_semaphore()
    peers = [to_pair(q) for q in range(1, np_)] + [to_x(q) for q in range(1, nx)] + [to_z(q) for q in range(1, nz)]
    for peer in peers:
        pl.semaphore_signal(barrier, inc=1, device_id=peer, device_id_type=pl.DeviceIdType.MESH)

    loads = [pltpu.make_async_copy(act_hbm, act_ref, load.at[0]), pltpu.make_async_copy(cot_hbm, cot_ref, load.at[1])]
    for copy in loads:
        copy.start()
    loads[0].wait()
    act_t[...] = act_ref[...].T
    loads[1].wait()
    width = 2 if nc % 2 == 0 else 1

    def compute(g):
        for xi in range(nx):
            col = pl.multiple_of(xi * cols_x + g * (width * LANES), LANES)
            grad = jnp.dot(act_t[...], cot_ref[:, pl.ds(col, width * LANES)], preferred_element_type=jnp.float32)
            for w in range(width):
                for pi in range(np_):
                    for zi in range(nz):
                        for s in range(ns):
                            row = pi * rows_p + (zi * ns + s) * rs
                            part[(g * width + w) * ns + s, pi, xi, zi] = grad[row:row + rs, w * LANES:(w + 1) * LANES]

    groups = nc // width
    early = max(1, groups // 2)
    pl.loop(0, early)(compute)
    pl.semaphore_wait(barrier, len(peers))
    ahead = min(AHEAD, early * width * ns)
    for k in range(ahead):
        start_first(k)
    pl.loop(early, groups)(compute)

    @pl.loop(0, chunks + LAG[2])
    def _(t):
        pl.when(t + ahead < chunks)(lambda: start_first(t + ahead))
        pl.when(t < chunks)(lambda: stage2(t))
        pl.when((t >= LAG[0]) & (t - LAG[0] < chunks))(lambda: stage3(t - LAG[0]))
        pl.when((t >= LAG[1]) & (t - LAG[1] < chunks))(lambda: stage4(t - LAG[1]))
        pl.when(t >= LAG[2])(lambda: stage5(t - LAG[2]))

    @pl.loop(0, chunks)
    def _(k):
        stage6(k)
        finish(k)


def solution(mesh):
    np_, ndp = mesh.shape["pair"], mesh.shape["dp"]
    nx = 1
    while (2 * nx) ** 2 <= ndp and ndp % (2 * nx) == 0:
        nx *= 2
    nz = ndp // nx

    def local(activations, cotangents):
        rows, cols = activations.shape[1], cotangents.shape[1]
        nc = cols // nx // LANES
        ns = SPLIT
        rs = rows // np_ // nz // ns
        chunks = nc * ns
        wide = max(np_, nx)
        f32, bf16 = jnp.float32, jnp.bfloat16
        dma = pltpu.SemaphoreType.DMA
        return pl.pallas_call(
            functools.partial(kernel, np_, nx, nz, nc, ns),
            out_shape=jax.ShapeDtypeStruct((rows // np_, cols), jnp.bfloat16),
            in_specs=[pl.BlockSpec(memory_space=pltpu.HBM)] * 2,
            out_specs=pl.BlockSpec(memory_space=pltpu.VMEM),
            scratch_shapes=[
                pltpu.VMEM(activations.shape, activations.dtype),
                pltpu.VMEM(cotangents.shape, cotangents.dtype),
                pltpu.VMEM((rows, activations.shape[0]), activations.dtype),
                pltpu.VMEM((chunks, np_, nx, nz, rs, LANES), f32),
                pltpu.VMEM((chunks, np_, nx, nz, rs, LANES), bf16),
                pltpu.VMEM((chunks, np_ * nx, nz, rs, LANES), bf16),
                pltpu.VMEM((chunks, wide, nz, rs, LANES), bf16),
                pltpu.VMEM((chunks, nz, rs, LANES), bf16),
                dma((chunks, wide)), dma((chunks, wide)),
                dma((chunks, wide)), dma((chunks, wide)),
                dma((chunks, nz)), dma((chunks, nz)),
                dma((chunks, nz)), dma((chunks, nz)),
                dma((chunks, nz, nx)), dma((chunks, nz, nx)),
                dma((2,)),
            ],
            compiler_params=pltpu.CompilerParams(
                collective_id=0, has_side_effects=True, vmem_limit_bytes=60 * 1024 * 1024),
        )(activations, cotangents)

    in_specs = (P(("pair", "dp"), "ep"), P(("pair", "dp"), "ep"))
    return jax.shard_map(local, mesh=mesh, in_specs=in_specs, out_specs=P("pair", "ep"), check_vma=False)
```

```python
import functools
import math

import jax
import jax.numpy as jnp
from jax import lax
from jax.experimental import pallas as pl
from jax.experimental.pallas import tpu as pltpu
from jax.sharding import PartitionSpec as P

LANES = 128
SPLIT = 2
POWER = 11
LARGEST_PRODUCT = 16 * 1.75
VM = 20
Y_FIRST = "AB"
X_GATHER = "0"
AHEAD = 8
LAGS = (0, 3, 7, 11, 12, 15)


def scale_and_offset(terms):
    scale = 2.0 ** math.floor(126 / POWER - math.log2(terms * LARGEST_PRODUCT))
    return scale, 2.0 ** (-124 / POWER)


def encode(x, terms):
    scale, offset = scale_and_offset(terms)
    a = x * scale + jnp.where(x < 0, -offset, offset)
    a2 = a * a
    a4 = a2 * a2
    return (a4 * a4 * (a2 * a)).astype(jnp.bfloat16)


def decode(f, terms):
    scale, offset = scale_and_offset(terms)
    f = f.astype(jnp.float32)
    a = jnp.exp2(jnp.log2(jnp.abs(f)) * (1 / POWER) - math.log2(scale)) - offset / scale
    return jnp.where(f < 0, -a, a)


def kernel(np_, nx, nz, nc, ns, act_hbm, cot_hbm, out_ref, act_ref, cot_ref, act_t, part, enc, f1, f2, zr,
           s1, r1, s2, r2, sz, rz, sgz, sgx, sr, rn, rf, rl, load):
    p = lax.axis_index("pair")
    dp = lax.axis_index("dp")
    z, x = dp // nx, dp % nx
    rs = part.shape[-2]
    chunks = nc * ns
    rows_p = nz * ns * rs
    cols_x = nc * LANES
    terms = act_ref.shape[0]
    replicas = np_ * nx * nz
    half = max(1, nz // 2)
    low = z < half
    base = jnp.where(low, 0, half)
    far = jnp.where(low, half, 0)
    gateway = jnp.where(low, half - 1, half)
    opposite = jnp.where(low, half, half - 1)

    def other(i, q, n):
        return lax.rem(i + q, n)

    def to_pair(q):
        return {"pair": other(p, q, np_)}

    def to_x(q):
        return {"dp": z * nx + other(x, q, nx)}

    def at_z(zi):
        return {"dp": zi * nx + x}

    def near(q):
        return base + other(z - base, q, half)

    def y_first(k):
        return Y_FIRST[k % len(Y_FIRST)] == "A"

    def x_gather(k):
        return int(X_GATHER[k % len(X_GATHER)])

    def remote(src, dst, ssem, rsem, peer):
        return pltpu.make_async_remote_copy(
            src_ref=src, dst_ref=dst, send_sem=ssem, recv_sem=rsem,
            device_id=peer, device_id_type=pl.DeviceIdType.MESH)

    def arrived(ref, rsem):
        remote(ref, ref, rsem, rsem, to_pair(1)).wait_recv()

    def sent(ref, ssem):
        remote(ref, ref, ssem, ssem, to_pair(1)).wait_send()

    def piece(k, zi, xi):
        c, s = k // ns, k % ns
        row = pl.multiple_of((zi * ns + s) * rs, rs)
        col = pl.multiple_of(xi * cols_x + c * LANES, LANES)
        return out_ref.at[pl.ds(row, rs), pl.ds(col, LANES)]

    def spread(k, zi, xi, peer, ssem, rsem):
        here = piece(k, zi, xi)
        remote(here, here, ssem, rsem, peer).start()

    def gather_z(k, xi):
        t = x_gather(k)
        if nz > 1:
            spread(k, z, xi, at_z(opposite), sgz.at[t], rf.at[k])
        for q in range(1, half):
            spread(k, z, xi, at_z(near(q)), sgz.at[t], rl.at[1] if t else rn.at[k])

    def gather_x(k, zi):
        t = x_gather(k)
        for q in range(1, nx):
            spread(k, zi, x, to_x(q), sgx.at[t], rn.at[k] if t else rl.at[0])

    def stage_first(k):
        if y_first(k):
            for q in range(1, np_):
                o = other(p, q, np_)
                enc[k, o] = encode(part[k, o], terms)
                remote(enc.at[k, o], f1.at[k, pl.ds(p * nx, nx)], s1.at[0], r1.at[k], to_pair(q)).start()
        else:
            for q in range(1, nx):
                o = other(x, q, nx)
                enc[k, :, o] = encode(part[k, :, o], terms)
                remote(enc.at[k, :, o], f1.at[k, pl.ds(x * np_, np_)], s1.at[1], r1.at[k], to_x(q)).start()

    def stage_second(k):
        if y_first(k):
            arrived(f1.at[k, pl.ds(0, (np_ - 1) * nx)], r1.at[k])
            for q in range(1, np_):
                o = other(p, q, np_)
                part[k, p] += decode(f1[k, pl.ds(o * nx, nx)], terms)
            for q in range(1, nx):
                o = other(x, q, nx)
                enc[k, p, o] = encode(part[k, p, o], np_ * terms)
                remote(enc.at[k, p, o], f2.at[k, x], s2.at[0], r2.at[k], to_x(q)).start()
        else:
            arrived(f1.at[k, pl.ds(0, (nx - 1) * np_)], r1.at[k])
            for q in range(1, nx):
                o = other(x, q, nx)
                part[k, :, x] += decode(f1[k, pl.ds(o * np_, np_)], terms)
            for q in range(1, np_):
                o = other(p, q, np_)
                enc[k, o, x] = encode(part[k, o, x], nx * terms)
                remote(enc.at[k, o, x], f2.at[k, p], s2.at[1], r2.at[k], to_pair(q)).start()

    def stage_third(k):
        n, i, count = (nx, x, np_) if y_first(k) else (np_, p, nx)
        arrived(f2.at[k, pl.ds(0, n - 1)], r2.at[k])
        for q in range(1, n):
            part[k, p, x] += decode(f2[k, other(i, q, n)], count * terms)
        for q in range(1, nz):
            o = other(z, q, nz)
            enc[k, p, x, o] = encode(part[k, p, x, o], np_ * nx * terms)
            remote(enc.at[k, p, x, o], zr.at[k, z], sz, rz.at[k], at_z(o)).start()

    def stage_own(k):
        total = part[k, p, x, z]
        if nz > 1:
            arrived(zr.at[k, pl.ds(0, nz - 1)], rz.at[k])
        for q in range(1, nz):
            total = total + decode(zr[k, other(z, q, nz)], np_ * nx * terms)
        piece(k, z, x)[...] = (total / replicas).astype(out_ref.dtype)
        if x_gather(k):
            gather_x(k, z)
            gather_z(k, x)
        else:
            gather_z(k, x)
            gather_x(k, z)

    def stage_near(k):
        if x_gather(k):
            arrived(enc.at[k, 0, pl.ds(0, nx - 1), 0], rn.at[k])
            for q in range(1, nx):
                gather_z(k, other(x, q, nx))
        elif half > 1:
            arrived(enc.at[k, 0, 0, pl.ds(0, half - 1)], rn.at[k])
            for q in range(1, half):
                gather_x(k, near(q))

    def far_bytes(k):
        return enc.at[k, 0, :, pl.ds(0, half)] if x_gather(k) else enc.at[k, 0, 0, pl.ds(0, half)]

    def stage_relay(k):
        t = x_gather(k)
        if half > 1:
            @pl.when(z == gateway)
            def _():
                arrived(far_bytes(k), rf.at[k])
                for j in range(half):
                    for xi in [x] + [other(x, q, nx) for q in range(1, nx if t else 1)]:
                        for q in range(1, half):
                            spread(k, far + j, xi, at_z(near(q)), sr.at[t, q], rf.at[k])

    def stage_far(k):
        if half > 1:
            @pl.when(z != gateway)
            def _():
                arrived(far_bytes(k), rf.at[k])
        elif nz > 1:
            arrived(far_bytes(k), rf.at[k])
        if nz > 1 and not x_gather(k):
            for j in range(half):
                gather_x(k, far + j)

    def drain():
        kinds = [sum(1 for k in range(chunks) if not y_first(k)), sum(1 for k in range(chunks) if x_gather(k))]
        a, b = chunks - kinds[0], kinds[0]
        g0, g1 = chunks - kinds[1], kinds[1]
        if a:
            sent(enc.at[pl.ds(0, a), pl.ds(0, np_ - 1)], s1.at[0])
            sent(enc.at[pl.ds(0, a), 0, pl.ds(0, nx - 1)], s2.at[0])
        if b:
            sent(enc.at[pl.ds(0, b), :, pl.ds(0, nx - 1)], s1.at[1])
            sent(enc.at[pl.ds(0, b), pl.ds(0, np_ - 1), 0], s2.at[1])
        if nz > 1:
            sent(enc.at[:, 0, 0, pl.ds(0, nz - 1)], sz)
        for t, g in ((0, g0), (1, g1)):
            if not g:
                continue
            if nz > 1:
                wide = enc.at[pl.ds(0, g), 0, :, pl.ds(0, half)] if t else enc.at[pl.ds(0, g), 0, 0, pl.ds(0, half)]
                sent(wide, sgz.at[t])
                if half > 1:
                    @pl.when(z == gateway)
                    def _():
                        for q in range(1, half):
                            sent(wide, sr.at[t, q])
            if t:
                sent(enc.at[pl.ds(0, g), 0, pl.ds(0, nx - 1), 0], sgx.at[t])
                if half > 1:
                    arrived(enc.at[pl.ds(0, g), 0, :, pl.ds(0, half - 1)], rl.at[t])
            else:
                sent(enc.at[pl.ds(0, g), 0, pl.ds(0, nx - 1)], sgx.at[t])
                arrived(enc.at[pl.ds(0, g), 0, pl.ds(0, nx - 1)], rl.at[t])

    barrier = pltpu.get_barrier_semaphore()
    peers = [to_pair(q) for q in range(1, np_)] + [to_x(q) for q in range(1, nx)] + [at_z(other(z, q, nz)) for q in range(1, nz)]
    for peer in peers:
        pl.semaphore_signal(barrier, inc=1, device_id=peer, device_id_type=pl.DeviceIdType.MESH)

    width = 2 if nc % 2 == 0 else 1
    groups = nc // width
    blocks = [(g, xi) for g in range(groups) for xi in range(nx)]

    def block(g, xi):
        return pl.ds(xi * cols_x + g * (width * LANES), width * LANES)

    loads = [pltpu.make_async_copy(act_hbm, act_ref, load.at[len(blocks)])]
    loads += [pltpu.make_async_copy(cot_hbm.at[:, block(g, xi)], cot_ref.at[:, block(g, xi)], load.at[i])
              for i, (g, xi) in enumerate(blocks)]
    for copy in loads:
        copy.start()
    loads[0].wait()
    act_t[...] = act_ref[...].T

    def compute(g):
        for xi in range(nx):
            loads[1 + g * nx + xi].wait()
            grad = jnp.dot(act_t[...], cot_ref[:, block(g, xi)], preferred_element_type=jnp.float32)
            for w in range(width):
                for pi in range(np_):
                    for zi in range(nz):
                        for s in range(ns):
                            row = pi * rows_p + (zi * ns + s) * rs
                            part[(g * width + w) * ns + s, pi, xi, zi] = grad[row:row + rs, w * LANES:(w + 1) * LANES]

    per = width * ns
    stages = [stage_first, stage_second, stage_third, stage_own, stage_near, stage_relay, stage_far]
    lags = (-AHEAD,) + LAGS
    events = sorted((k + lags[i], -i, k) for k in range(chunks) for i in range(len(stages)))
    done = 0
    waited = False
    for _, i, k in events:
        while done <= k // per:
            compute(done)
            done += 1
        if not waited:
            pl.semaphore_wait(barrier, len(peers))
            waited = True
        stages[-i](k)
    drain()


def solution(mesh):
    np_, ndp = mesh.shape["pair"], mesh.shape["dp"]
    nx = 1
    while (2 * nx) ** 2 <= ndp and ndp % (2 * nx) == 0:
        nx *= 2
    nz = ndp // nx

    def local(activations, cotangents):
        rows, cols = activations.shape[1], cotangents.shape[1]
        nc = cols // nx // LANES
        ns = SPLIT
        rs = rows // np_ // nz // ns
        chunks = nc * ns
        wide = max(np_, nx)
        f32, bf16 = jnp.float32, jnp.bfloat16
        dma = pltpu.SemaphoreType.DMA
        activations, cotangents = (pltpu.with_memory_space_constraint(a, pltpu.HBM) for a in (activations, cotangents))
        return pl.pallas_call(
            functools.partial(kernel, np_, nx, nz, nc, ns),
            out_shape=jax.ShapeDtypeStruct((rows // np_, cols), jnp.bfloat16),
            in_specs=[pl.BlockSpec(memory_space=pltpu.HBM)] * 2,
            out_specs=pl.BlockSpec(memory_space=pltpu.VMEM),
            scratch_shapes=[
                pltpu.VMEM(activations.shape, activations.dtype),
                pltpu.VMEM(cotangents.shape, cotangents.dtype),
                pltpu.VMEM((rows, activations.shape[0]), activations.dtype),
                pltpu.VMEM((chunks, np_, nx, nz, rs, LANES), f32),
                pltpu.VMEM((chunks, np_, nx, nz, rs, LANES), bf16),
                pltpu.VMEM((chunks, np_ * nx, nz, rs, LANES), bf16),
                pltpu.VMEM((chunks, wide, nz, rs, LANES), bf16),
                pltpu.VMEM((chunks, nz, rs, LANES), bf16),
                dma((2,)), dma((chunks,)), dma((2,)), dma((chunks,)), dma(()), dma((chunks,)),
                dma((2,)), dma((2,)), dma((2, nz)), dma((chunks,)), dma((chunks,)), dma((2,)),
                dma((1 + nc * nx,)),
            ],
            compiler_params=pltpu.CompilerParams(
                collective_id=0, has_side_effects=True, vmem_limit_bytes=VM * 1024 * 1024),
        )(activations, cotangents)

    in_specs = (P(("pair", "dp"), "ep"), P(("pair", "dp"), "ep"))
    return jax.shard_map(local, mesh=mesh, in_specs=in_specs, out_specs=P("pair", "ep"), check_vma=False)
```

```python
import functools
import math

import jax
import jax.numpy as jnp
from jax import lax
from jax.experimental import pallas as pl
from jax.experimental.pallas import tpu as pltpu
from jax.sharding import PartitionSpec as P

LANES = 128
SPLIT = 2
POWER = 11
LARGEST_PRODUCT = 16 * 1.75
VM = 20
KINDS = "CCCABABABABABABA"
CSLOTS = (-9, 6, 11, 15, 19, 20, 24, 2)
CSTEP = 2
RATE = 1
SA = 2
SB = 2
OB = 1
X_GATHER = "0"
AHEAD = 4
LAGS = (0, 4, 9, 14, 15, 19)
XLAGS = (12, 17, 21)


def scale_and_offset(terms):
    scale = 2.0 ** math.floor(126 / POWER - math.log2(terms * LARGEST_PRODUCT))
    return scale, 2.0 ** (-124 / POWER)


def encode(x, terms):
    scale, offset = scale_and_offset(terms)
    a = x * scale + jnp.where(x < 0, -offset, offset)
    a2 = a * a
    a4 = a2 * a2
    return (a4 * a4 * (a2 * a)).astype(jnp.bfloat16)


def decode(f, terms):
    scale, offset = scale_and_offset(terms)
    f = f.astype(jnp.float32)
    a = jnp.exp2(jnp.log2(jnp.abs(f)) * (1 / POWER) - math.log2(scale)) - offset / scale
    return jnp.where(f < 0, -a, a)


def kernel(np_, nx, nz, nc, ns, act_hbm, cot_hbm, out_ref, act_ref, cot_ref, act_t, part, enc, f1, f2, zr, fc, fg, fy, fx,
           s1, r1, rg, s2, r2, sz, rz, sgz, sgx, sr, rn, rf, rl, load):
    p = lax.axis_index("pair")
    dp = lax.axis_index("dp")
    z, x = dp // nx, dp % nx
    rs = part.shape[-2]
    chunks = nc * ns
    rows_p = nz * ns * rs
    cols_x = nc * LANES
    terms = act_ref.shape[0]
    replicas = np_ * nx * nz
    half = max(1, nz // 2)
    low = z < half
    base = jnp.where(low, 0, half)
    far = jnp.where(low, half, 0)
    gateway = jnp.where(low, half - 1, half)
    opposite = jnp.where(low, half, half - 1)

    def other(i, q, n):
        return lax.rem(i + q, n)

    def to_pair(q):
        return {"pair": other(p, q, np_)}

    def to_x(q):
        return {"dp": z * nx + other(x, q, nx)}

    def at_z(zi):
        return {"dp": zi * nx + x}

    def near(q):
        return base + other(z - base, q, half)

    def kind(k):
        return KINDS[k % len(KINDS)]

    def x_gather(k):
        return int(X_GATHER[k % len(X_GATHER)])

    def remote(src, dst, ssem, rsem, peer):
        return pltpu.make_async_remote_copy(
            src_ref=src, dst_ref=dst, send_sem=ssem, recv_sem=rsem,
            device_id=peer, device_id_type=pl.DeviceIdType.MESH)

    def arrived(ref, rsem):
        remote(ref, ref, rsem, rsem, to_pair(1)).wait_recv()

    def sent(ref, ssem):
        remote(ref, ref, ssem, ssem, to_pair(1)).wait_send()

    def piece(k, zi, xi):
        c, s = k // ns, k % ns
        row = pl.multiple_of((zi * ns + s) * rs, rs)
        col = pl.multiple_of(xi * cols_x + c * LANES, LANES)
        return out_ref.at[pl.ds(row, rs), pl.ds(col, LANES)]

    def spread(k, zi, xi, peer, ssem, rsem):
        here = piece(k, zi, xi)
        remote(here, here, ssem, rsem, peer).start()

    def gather_z(k, xi):
        t = x_gather(k)
        if nz > 1:
            spread(k, z, xi, at_z(opposite), sgz.at[t], rf.at[k])
        for q in range(1, half):
            spread(k, z, xi, at_z(near(q)), sgz.at[t], rl.at[1] if t else rn.at[k])

    def gather_x(k, zi):
        t = x_gather(k)
        for q in range(1, nx):
            spread(k, zi, x, to_x(q), sgx.at[t], rn.at[k] if t else rl.at[0])

    cs = [k for k in range(chunks) if kind(k) == "C"]

    def stage_first(k):
        if kind(k) == "C":
            c = cs.index(k)
            if half > 1:
                @pl.when(z != gateway)
                def _():
                    for j in range(half):
                        enc[k, :, :, far + j] = encode(part[k, :, :, far + j], terms)
                        remote(enc.at[k, :, :, far + j], fg.at[c, z - base, j], s1.at[3], rg.at[c], at_z(gateway)).start()
            for q in range(1, half):
                o = near(q)
                enc[k, :, :, o] = encode(part[k, :, :, o], terms)
                remote(enc.at[k, :, :, o], fc.at[c, z], s1.at[2], r1.at[k], at_z(o)).start()
        elif kind(k) == "A":
            for q in range(1, np_):
                o = other(p, q, np_)
                enc[k, o] = encode(part[k, o], terms)
                remote(enc.at[k, o], f1.at[k, pl.ds(p * nx, nx)], s1.at[0], r1.at[k], to_pair(q)).start()
        else:
            for q in range(1, nx):
                o = other(x, q, nx)
                enc[k, :, o] = encode(part[k, :, o], terms)
                remote(enc.at[k, :, o], f1.at[k, pl.ds(x * np_, np_)], s1.at[1], r1.at[k], to_x(q)).start()

    def stage_pre(k):
        c = cs.index(k)

        @pl.when(z == gateway)
        def _():
            if half > 1:
                arrived(fg.at[c, pl.ds(0, half - 1)], rg.at[c])
            for j in range(half):
                total = part[k, :, :, far + j]
                for q in range(1, half):
                    total = total + decode(fg[c, near(q) - base, j], terms)
                enc[k, :, :, far + j] = encode(total, half * terms)
                remote(enc.at[k, :, :, far + j], fc.at[c, base], s1.at[3], r1.at[k], at_z(far + j)).start()

    def stage_second(k):
        if kind(k) == "C":
            c = cs.index(k)
            arrived(fc.at[c, pl.ds(0, half)], r1.at[k])
            part[k, :, :, z] += decode(fc[c, far], half * terms)
            for q in range(1, half):
                part[k, :, :, z] += decode(fc[c, near(q)], terms)
            for q in range(1, np_):
                o = other(p, q, np_)
                enc[k, o, :, z] = encode(part[k, o, :, z], nz * terms)
                remote(enc.at[k, o, :, z], fy.at[cs.index(k), p], s2.at[2], r2.at[k], to_pair(q)).start()
        elif kind(k) == "A":
            arrived(f1.at[k, pl.ds(0, (np_ - 1) * nx)], r1.at[k])
            for q in range(1, np_):
                o = other(p, q, np_)
                part[k, p] += decode(f1[k, pl.ds(o * nx, nx)], terms)
            for q in range(1, nx):
                o = other(x, q, nx)
                enc[k, p, o] = encode(part[k, p, o], np_ * terms)
                remote(enc.at[k, p, o], f2.at[k, x], s2.at[0], r2.at[k], to_x(q)).start()
        else:
            arrived(f1.at[k, pl.ds(0, (nx - 1) * np_)], r1.at[k])
            for q in range(1, nx):
                o = other(x, q, nx)
                part[k, :, x] += decode(f1[k, pl.ds(o * np_, np_)], terms)
            for q in range(1, np_):
                o = other(p, q, np_)
                enc[k, o, x] = encode(part[k, o, x], nx * terms)
                remote(enc.at[k, o, x], f2.at[k, p], s2.at[1], r2.at[k], to_pair(q)).start()

    def stage_third(k):
        if kind(k) == "C":
            arrived(fy.at[cs.index(k), pl.ds(0, np_ - 1)], r2.at[k])
            for q in range(1, np_):
                part[k, p, :, z] += decode(fy[cs.index(k), other(p, q, np_)], nz * terms)
            for q in range(1, nx):
                o = other(x, q, nx)
                enc[k, p, o, z] = encode(part[k, p, o, z], np_ * nz * terms)
                remote(enc.at[k, p, o, z], fx.at[cs.index(k), x], sz.at[1], rz.at[k], to_x(q)).start()
            return
        n, i, count = (nx, x, np_) if kind(k) == "A" else (np_, p, nx)
        arrived(f2.at[k, pl.ds(0, n - 1)], r2.at[k])
        for q in range(1, n):
            part[k, p, x] += decode(f2[k, other(i, q, n)], count * terms)
        for q in range(1, nz):
            o = other(z, q, nz)
            enc[k, p, x, o] = encode(part[k, p, x, o], np_ * nx * terms)
            remote(enc.at[k, p, x, o], zr.at[k, z], sz.at[0], rz.at[k], at_z(o)).start()

    def stage_own(k):
        total = part[k, p, x, z]
        if kind(k) == "C":
            arrived(fx.at[cs.index(k), pl.ds(0, nx - 1)], rz.at[k])
            for q in range(1, nx):
                total = total + decode(fx[cs.index(k), other(x, q, nx)], np_ * nz * terms)
        elif nz > 1:
            arrived(zr.at[k, pl.ds(0, nz - 1)], rz.at[k])
        for q in range(1, nz if kind(k) != "C" else 1):
            total = total + decode(zr[k, other(z, q, nz)], np_ * nx * terms)
        piece(k, z, x)[...] = (total / replicas).astype(out_ref.dtype)
        if x_gather(k):
            gather_x(k, z)
            gather_z(k, x)
        else:
            gather_z(k, x)
            gather_x(k, z)

    def stage_near(k):
        if x_gather(k):
            arrived(enc.at[k, 0, pl.ds(0, nx - 1), 0], rn.at[k])
            for q in range(1, nx):
                gather_z(k, other(x, q, nx))
        elif half > 1:
            arrived(enc.at[k, 0, 0, pl.ds(0, half - 1)], rn.at[k])
            for q in range(1, half):
                gather_x(k, near(q))

    def far_bytes(k):
        return enc.at[k, 0, :, pl.ds(0, half)] if x_gather(k) else enc.at[k, 0, 0, pl.ds(0, half)]

    def stage_relay(k):
        t = x_gather(k)
        if half > 1:
            @pl.when(z == gateway)
            def _():
                arrived(far_bytes(k), rf.at[k])
                for j in range(half):
                    for xi in [x] + [other(x, q, nx) for q in range(1, nx if t else 1)]:
                        for q in range(1, half):
                            spread(k, far + j, xi, at_z(near(q)), sr.at[t, q], rf.at[k])

    def stage_far(k):
        if half > 1:
            @pl.when(z != gateway)
            def _():
                arrived(far_bytes(k), rf.at[k])
        elif nz > 1:
            arrived(far_bytes(k), rf.at[k])
        if nz > 1 and not x_gather(k):
            for j in range(half):
                gather_x(k, far + j)

    def drain():
        a, b, c = (sum(kind(k) == t for k in range(chunks)) for t in "ABC")
        g1 = sum(x_gather(k) for k in range(chunks))
        g0 = chunks - g1
        if a:
            sent(enc.at[pl.ds(0, a), pl.ds(0, np_ - 1)], s1.at[0])
            sent(enc.at[pl.ds(0, a), 0, pl.ds(0, nx - 1)], s2.at[0])
        if b:
            sent(enc.at[pl.ds(0, b), :, pl.ds(0, nx - 1)], s1.at[1])
            sent(enc.at[pl.ds(0, b), pl.ds(0, np_ - 1), 0], s2.at[1])
        if c:
            if half > 1:
                sent(enc.at[pl.ds(0, c), :, :, pl.ds(0, half - 1)], s1.at[2])
            sent(enc.at[pl.ds(0, c), :, :, pl.ds(0, half)], s1.at[3])
            sent(enc.at[pl.ds(0, c), pl.ds(0, np_ - 1), :, 0], s2.at[2])
            sent(enc.at[pl.ds(0, c), 0, pl.ds(0, nx - 1), 0], sz.at[1])
        if nz > 1 and a + b:
            sent(enc.at[pl.ds(0, a + b), 0, 0, pl.ds(0, nz - 1)], sz.at[0])
        for t, g in ((0, g0), (1, g1)):
            if not g:
                continue
            if nz > 1:
                wide = enc.at[pl.ds(0, g), 0, :, pl.ds(0, half)] if t else enc.at[pl.ds(0, g), 0, 0, pl.ds(0, half)]
                sent(wide, sgz.at[t])
                if half > 1:
                    @pl.when(z == gateway)
                    def _():
                        for q in range(1, half):
                            sent(wide, sr.at[t, q])
            if t:
                sent(enc.at[pl.ds(0, g), 0, pl.ds(0, nx - 1), 0], sgx.at[t])
                if half > 1:
                    arrived(enc.at[pl.ds(0, g), 0, :, pl.ds(0, half - 1)], rl.at[t])
            else:
                sent(enc.at[pl.ds(0, g), 0, pl.ds(0, nx - 1)], sgx.at[t])
                arrived(enc.at[pl.ds(0, g), 0, pl.ds(0, nx - 1)], rl.at[t])

    barrier = pltpu.get_barrier_semaphore()
    peers = [to_pair(q) for q in range(1, np_)] + [to_x(q) for q in range(1, nx)] + [at_z(other(z, q, nz)) for q in range(1, nz)]
    for peer in peers:
        pl.semaphore_signal(barrier, inc=1, device_id=peer, device_id_type=pl.DeviceIdType.MESH)

    width = 2 if nc % 2 == 0 else 1
    groups = nc // width
    blocks = [(g, xi) for g in range(groups) for xi in range(nx)]

    def block(g, xi):
        return pl.ds(xi * cols_x + g * (width * LANES), width * LANES)

    def held(xi):
        return pl.ds(xi * (width * LANES), width * LANES)

    loads = [pltpu.make_async_copy(act_hbm, act_ref, load.at[len(blocks)])]
    loads += [pltpu.make_async_copy(cot_hbm.at[:, block(g, xi)], cot_ref.at[g, :, held(xi)], load.at[i])
              for i, (g, xi) in enumerate(blocks)]
    for copy in loads:
        copy.start()
    loads[0].wait()
    act_t[...] = act_ref[...].T

    def compute(g):
        for xi in range(nx):
            loads[1 + g * nx + xi].wait()
        grad = jnp.dot(act_t[...], cot_ref[g], preferred_element_type=jnp.float32)
        for xi in range(nx):
            for w in range(width):
                col = (xi * width + w) * LANES
                for pi in range(np_):
                    for zi in range(nz):
                        for s in range(ns):
                            row = pi * rows_p + (zi * ns + s) * rs
                            part[(g * width + w) * ns + s, pi, xi, zi] = grad[row:row + rs, col:col + LANES]

    per = width * ns
    stages = [stage_first, stage_second, stage_third, stage_own, stage_near, stage_relay, stage_far, stage_pre]
    lags = ((-AHEAD,) + LAGS, (-AHEAD,) + LAGS[:3] + XLAGS)
    events = []
    for k in range(chunks):
        if kind(k) == "C":
            j = cs.index(k)
            slots = [CSLOTS[0]] + [slot + CSTEP * j for slot in CSLOTS[1:]]
        else:
            j = sum(kind(i) == kind(k) for i in range(k)) * (SA if kind(k) == "A" else SB) + (0 if kind(k) == "A" else OB)
            slots = [RATE * j - AHEAD] + [j + lag for lag in lags[x_gather(k)][1:]]
        events += [(slot, -i, k) for i, slot in enumerate(slots)]
    events.sort()
    done = 0
    waited = False
    for _, i, k in events:
        while done < groups and (done <= k // per or -i not in (0, 7)):
            compute(done)
            done += 1
        if not waited:
            pl.semaphore_wait(barrier, len(peers))
            waited = True
        stages[-i](k)
    drain()


def solution(mesh):
    np_, ndp = mesh.shape["pair"], mesh.shape["dp"]
    nx = 1
    while (2 * nx) ** 2 <= ndp and ndp % (2 * nx) == 0:
        nx *= 2
    nz = ndp // nx

    def local(activations, cotangents):
        rows, cols = activations.shape[1], cotangents.shape[1]
        nc = cols // nx // LANES
        ns = SPLIT
        width = 2 if nc % 2 == 0 else 1
        rs = rows // np_ // nz // ns
        chunks = nc * ns
        wide = max(np_, nx)
        half = max(1, nz // 2)
        cs = max(1, sum(KINDS[k % len(KINDS)] == "C" for k in range(chunks)))
        f32, bf16 = jnp.float32, jnp.bfloat16
        dma = pltpu.SemaphoreType.DMA
        activations, cotangents = (pltpu.with_memory_space_constraint(a, pltpu.HBM) for a in (activations, cotangents))
        return pl.pallas_call(
            functools.partial(kernel, np_, nx, nz, nc, ns),
            out_shape=jax.ShapeDtypeStruct((rows // np_, cols), jnp.bfloat16),
            in_specs=[pl.BlockSpec(memory_space=pltpu.HBM)] * 2,
            out_specs=pl.BlockSpec(memory_space=pltpu.VMEM),
            scratch_shapes=[
                pltpu.VMEM(activations.shape, activations.dtype),
                pltpu.VMEM((nc // width, cotangents.shape[0], nx * width * LANES), cotangents.dtype),
                pltpu.VMEM((rows, activations.shape[0]), activations.dtype),
                pltpu.VMEM((chunks, np_, nx, nz, rs, LANES), f32),
                pltpu.VMEM((chunks, np_, nx, nz, rs, LANES), bf16),
                pltpu.VMEM((chunks, np_ * nx, nz, rs, LANES), bf16),
                pltpu.VMEM((chunks, wide, nz, rs, LANES), bf16),
                pltpu.VMEM((chunks, nz, rs, LANES), bf16),
                pltpu.VMEM((cs, nz, np_, nx, rs, LANES), bf16),
                pltpu.VMEM((cs, half, half, np_, nx, rs, LANES), bf16),
                pltpu.VMEM((cs, np_, nx, rs, LANES), bf16),
                pltpu.VMEM((cs, nx, rs, LANES), bf16),
                dma((4,)), dma((chunks,)), dma((cs,)), dma((3,)), dma((chunks,)), dma((2,)), dma((chunks,)),
                dma((2,)), dma((2,)), dma((2, max(2, nz // 2))), dma((chunks,)), dma((chunks,)), dma((2,)),
                dma((1 + nc // width * nx,)),
            ],
            compiler_params=pltpu.CompilerParams(
                collective_id=0, has_side_effects=True, vmem_limit_bytes=VM * 1024 * 1024),
        )(activations, cotangents)

    in_specs = (P(("pair", "dp"), "ep"), P(("pair", "dp"), "ep"))
    return jax.shard_map(local, mesh=mesh, in_specs=in_specs, out_specs=P("pair", "ep"), check_vma=False)
```

```python
import functools
import math

import jax
import jax.numpy as jnp
from jax import lax
from jax.experimental import pallas as pl
from jax.experimental.pallas import tpu as pltpu
from jax.sharding import PartitionSpec as P

LANES = 128
SPLIT = 2
POWER = 11
LARGEST_PRODUCT = 16 * 1.75
VM = 20
KINDS = "CCCABABABABABABA"
CSLOTS = (-9, 6, 11, 15, 19, 20, 24, 2)
CSTEP = 2
RATE = 1
SA = 2
SB = 2
OB = 1
DIRECT = 3
AHEAD = 5
LAGS = (0, 4, 9, 12, 13, 18)


def scale_and_offset(terms):
    scale = 2.0 ** math.floor(126 / POWER - math.log2(terms * LARGEST_PRODUCT))
    return scale, 2.0 ** (-124 / POWER)


def encode(x, terms):
    scale, offset = scale_and_offset(terms)
    a = x * scale + jnp.where(x < 0, -offset, offset)
    a2 = a * a
    a4 = a2 * a2
    return (a4 * a4 * (a2 * a)).astype(jnp.bfloat16)


def decode(f, terms):
    scale, offset = scale_and_offset(terms)
    f = f.astype(jnp.float32)
    a = jnp.exp2(jnp.log2(jnp.abs(f)) * (1 / POWER) - math.log2(scale)) - offset / scale
    return jnp.where(f < 0, -a, a)


def kernel(np_, nx, nz, nc, ns, act_hbm, cot_hbm, out_ref, act_ref, cot_ref, act_t, part, enc, f1, f2, zr, fc, fg, fy, fx,
           s1, r1, rg, s2, r2, sz, rz, sgz, sgx, sr, rn, rf, rl, load):
    p = lax.axis_index("pair")
    dp = lax.axis_index("dp")
    z, x = dp // nx, dp % nx
    rs = part.shape[-2]
    chunks = nc * ns
    rows_p = nz * ns * rs
    cols_x = nc * LANES
    terms = act_ref.shape[0]
    replicas = np_ * nx * nz
    half = max(1, nz // 2)
    low = z < half
    base = jnp.where(low, 0, half)
    far = jnp.where(low, half, 0)
    gateway = jnp.where(low, half - 1, half)
    opposite = jnp.where(low, half, half - 1)

    def other(i, q, n):
        return lax.rem(i + q, n)

    def to_pair(q):
        return {"pair": other(p, q, np_)}

    def to_x(q):
        return {"dp": z * nx + other(x, q, nx)}

    def at_z(zi):
        return {"dp": zi * nx + x}

    def near(q):
        return base + other(z - base, q, half)

    def kind(k):
        return KINDS[k % len(KINDS)]

    def direct(k):
        return k >= chunks - DIRECT

    def remote(src, dst, ssem, rsem, peer):
        return pltpu.make_async_remote_copy(
            src_ref=src, dst_ref=dst, send_sem=ssem, recv_sem=rsem,
            device_id=peer, device_id_type=pl.DeviceIdType.MESH)

    def arrived(ref, rsem):
        remote(ref, ref, rsem, rsem, to_pair(1)).wait_recv()

    def sent(ref, ssem):
        remote(ref, ref, ssem, ssem, to_pair(1)).wait_send()

    def piece(k, zi, xi):
        c, s = k // ns, k % ns
        row = pl.multiple_of((zi * ns + s) * rs, rs)
        col = pl.multiple_of(xi * cols_x + c * LANES, LANES)
        return out_ref.at[pl.ds(row, rs), pl.ds(col, LANES)]

    def spread(k, zi, xi, peer, ssem, rsem):
        here = piece(k, zi, xi)
        remote(here, here, ssem, rsem, peer).start()

    def gather_z(k):
        if nz > 1:
            spread(k, z, x, at_z(opposite), sgz.at[0], rf.at[k])
        for q in range(1, half):
            spread(k, z, x, at_z(near(q)), sgz.at[0], rn.at[k])

    def gather_x(k, zi):
        for q in range(1, nx):
            spread(k, zi, x, to_x(q), sgx.at[0], rl.at[0])

    def gather_all(k):
        for zo in range(nz):
            for q in range(nx):
                peer = {"dp": other(z, zo, nz) * nx + other(x, q, nx)}
                if q:
                    spread(k, z, x, peer, sgx.at[1], rl.at[1])
                elif zo:
                    spread(k, z, x, peer, sgz.at[1], rl.at[2])

    cs = [k for k in range(chunks) if kind(k) == "C"]

    def stage_first(k):
        if kind(k) == "C":
            c = cs.index(k)
            if half > 1:
                @pl.when(z != gateway)
                def _():
                    for j in range(half):
                        enc[k, :, :, far + j] = encode(part[k, :, :, far + j], terms)
                        remote(enc.at[k, :, :, far + j], fg.at[c, z - base, j], s1.at[3], rg.at[c], at_z(gateway)).start()
            for q in range(1, half):
                o = near(q)
                enc[k, :, :, o] = encode(part[k, :, :, o], terms)
                remote(enc.at[k, :, :, o], fc.at[c, z], s1.at[2], r1.at[k], at_z(o)).start()
        elif kind(k) == "A":
            for q in range(1, np_):
                o = other(p, q, np_)
                enc[k, o] = encode(part[k, o], terms)
                remote(enc.at[k, o], f1.at[k, pl.ds(p * nx, nx)], s1.at[0], r1.at[k], to_pair(q)).start()
        else:
            for q in range(1, nx):
                o = other(x, q, nx)
                enc[k, :, o] = encode(part[k, :, o], terms)
                remote(enc.at[k, :, o], f1.at[k, pl.ds(x * np_, np_)], s1.at[1], r1.at[k], to_x(q)).start()

    def stage_pre(k):
        c = cs.index(k)

        @pl.when(z == gateway)
        def _():
            if half > 1:
                arrived(fg.at[c, pl.ds(0, half - 1)], rg.at[c])
            for j in range(half):
                total = part[k, :, :, far + j]
                for q in range(1, half):
                    total = total + decode(fg[c, near(q) - base, j], terms)
                enc[k, :, :, far + j] = encode(total, half * terms)
                remote(enc.at[k, :, :, far + j], fc.at[c, base], s1.at[3], r1.at[k], at_z(far + j)).start()

    def stage_second(k):
        if kind(k) == "C":
            c = cs.index(k)
            arrived(fc.at[c, pl.ds(0, half)], r1.at[k])
            part[k, :, :, z] += decode(fc[c, far], half * terms)
            for q in range(1, half):
                part[k, :, :, z] += decode(fc[c, near(q)], terms)
            for q in range(1, np_):
                o = other(p, q, np_)
                enc[k, o, :, z] = encode(part[k, o, :, z], nz * terms)
                remote(enc.at[k, o, :, z], fy.at[cs.index(k), p], s2.at[2], r2.at[k], to_pair(q)).start()
        elif kind(k) == "A":
            arrived(f1.at[k, pl.ds(0, (np_ - 1) * nx)], r1.at[k])
            for q in range(1, np_):
                o = other(p, q, np_)
                part[k, p] += decode(f1[k, pl.ds(o * nx, nx)], terms)
            for q in range(1, nx):
                o = other(x, q, nx)
                enc[k, p, o] = encode(part[k, p, o], np_ * terms)
                remote(enc.at[k, p, o], f2.at[k, x], s2.at[0], r2.at[k], to_x(q)).start()
        else:
            arrived(f1.at[k, pl.ds(0, (nx - 1) * np_)], r1.at[k])
            for q in range(1, nx):
                o = other(x, q, nx)
                part[k, :, x] += decode(f1[k, pl.ds(o * np_, np_)], terms)
            for q in range(1, np_):
                o = other(p, q, np_)
                enc[k, o, x] = encode(part[k, o, x], nx * terms)
                remote(enc.at[k, o, x], f2.at[k, p], s2.at[1], r2.at[k], to_pair(q)).start()

    def stage_third(k):
        if kind(k) == "C":
            arrived(fy.at[cs.index(k), pl.ds(0, np_ - 1)], r2.at[k])
            for q in range(1, np_):
                part[k, p, :, z] += decode(fy[cs.index(k), other(p, q, np_)], nz * terms)
            for q in range(1, nx):
                o = other(x, q, nx)
                enc[k, p, o, z] = encode(part[k, p, o, z], np_ * nz * terms)
                remote(enc.at[k, p, o, z], fx.at[cs.index(k), x], sz.at[1], rz.at[k], to_x(q)).start()
            return
        n, i, count = (nx, x, np_) if kind(k) == "A" else (np_, p, nx)
        arrived(f2.at[k, pl.ds(0, n - 1)], r2.at[k])
        for q in range(1, n):
            part[k, p, x] += decode(f2[k, other(i, q, n)], count * terms)
        for q in range(1, nz):
            o = other(z, q, nz)
            enc[k, p, x, o] = encode(part[k, p, x, o], np_ * nx * terms)
            remote(enc.at[k, p, x, o], zr.at[k, z], sz.at[0], rz.at[k], at_z(o)).start()

    def stage_own(k):
        total = part[k, p, x, z]
        if kind(k) == "C":
            arrived(fx.at[cs.index(k), pl.ds(0, nx - 1)], rz.at[k])
            for q in range(1, nx):
                total = total + decode(fx[cs.index(k), other(x, q, nx)], np_ * nz * terms)
        elif nz > 1:
            arrived(zr.at[k, pl.ds(0, nz - 1)], rz.at[k])
        for q in range(1, nz if kind(k) != "C" else 1):
            total = total + decode(zr[k, other(z, q, nz)], np_ * nx * terms)
        piece(k, z, x)[...] = (total / replicas).astype(out_ref.dtype)
        if direct(k):
            gather_all(k)
        else:
            gather_z(k)
            gather_x(k, z)

    def stage_near(k):
        if half > 1 and not direct(k):
            arrived(enc.at[k, 0, 0, pl.ds(0, half - 1)], rn.at[k])
            for q in range(1, half):
                gather_x(k, near(q))

    def stage_relay(k):
        if half > 1 and not direct(k):
            @pl.when(z == gateway)
            def _():
                arrived(enc.at[k, 0, 0, pl.ds(0, half)], rf.at[k])
                for j in range(half):
                    for q in range(1, half):
                        spread(k, far + j, x, at_z(near(q)), sr.at[q], rf.at[k])

    def stage_far(k):
        if nz == 1 or direct(k):
            return
        if half > 1:
            @pl.when(z != gateway)
            def _():
                arrived(enc.at[k, 0, 0, pl.ds(0, half)], rf.at[k])
        else:
            arrived(enc.at[k, 0, 0, pl.ds(0, half)], rf.at[k])
        for j in range(half):
            gather_x(k, far + j)

    def drain():
        a, b, c = (sum(kind(k) == t for k in range(chunks)) for t in "ABC")
        g1 = sum(direct(k) for k in range(chunks))
        g0 = chunks - g1
        if a:
            sent(enc.at[pl.ds(0, a), pl.ds(0, np_ - 1)], s1.at[0])
            sent(enc.at[pl.ds(0, a), 0, pl.ds(0, nx - 1)], s2.at[0])
        if b:
            sent(enc.at[pl.ds(0, b), :, pl.ds(0, nx - 1)], s1.at[1])
            sent(enc.at[pl.ds(0, b), pl.ds(0, np_ - 1), 0], s2.at[1])
        if c:
            if half > 1:
                sent(enc.at[pl.ds(0, c), :, :, pl.ds(0, half - 1)], s1.at[2])
            sent(enc.at[pl.ds(0, c), :, :, pl.ds(0, half)], s1.at[3])
            sent(enc.at[pl.ds(0, c), pl.ds(0, np_ - 1), :, 0], s2.at[2])
            sent(enc.at[pl.ds(0, c), 0, pl.ds(0, nx - 1), 0], sz.at[1])
        if nz > 1 and a + b:
            sent(enc.at[pl.ds(0, a + b), 0, 0, pl.ds(0, nz - 1)], sz.at[0])
        if g0:
            if nz > 1:
                group = enc.at[pl.ds(0, g0), 0, 0, pl.ds(0, half)]
                sent(group, sgz.at[0])
                if half > 1:
                    @pl.when(z == gateway)
                    def _():
                        for q in range(1, half):
                            sent(group, sr.at[q])
            if nx > 1:
                sent(enc.at[pl.ds(0, g0), 0, pl.ds(0, nx - 1)], sgx.at[0])
                arrived(enc.at[pl.ds(0, g0), 0, pl.ds(0, nx - 1)], rl.at[0])
        if g1:
            if nz > 1:
                sent(enc.at[pl.ds(0, g1), 0, 0, pl.ds(0, nz - 1)], sgz.at[1])
                arrived(enc.at[pl.ds(0, g1), 0, 0, pl.ds(0, nz - 1)], rl.at[2])
            if nx > 1:
                sent(enc.at[pl.ds(0, g1), 0, pl.ds(0, nx - 1)], sgx.at[1])
                arrived(enc.at[pl.ds(0, g1), 0, pl.ds(0, nx - 1)], rl.at[1])

    barrier = pltpu.get_barrier_semaphore()
    peers = [to_pair(q) for q in range(1, np_)] + [{"dp": other(dp, q, nz * nx)} for q in range(1, nz * nx)]
    for peer in peers:
        pl.semaphore_signal(barrier, inc=1, device_id=peer, device_id_type=pl.DeviceIdType.MESH)

    width = 2 if nc % 2 == 0 else 1
    groups = nc // width
    blocks = [(g, xi) for g in range(groups) for xi in range(nx)]

    def block(g, xi):
        return pl.ds(xi * cols_x + g * (width * LANES), width * LANES)

    def held(xi):
        return pl.ds(xi * (width * LANES), width * LANES)

    loads = [pltpu.make_async_copy(act_hbm, act_ref, load.at[len(blocks)])]
    loads += [pltpu.make_async_copy(cot_hbm.at[:, block(g, xi)], cot_ref.at[g, :, held(xi)], load.at[i])
              for i, (g, xi) in enumerate(blocks)]
    for copy in loads:
        copy.start()
    loads[0].wait()
    act_t[...] = act_ref[...].T

    def compute(g):
        for xi in range(nx):
            loads[1 + g * nx + xi].wait()
        grad = jnp.dot(act_t[...], cot_ref[g], preferred_element_type=jnp.float32)
        for xi in range(nx):
            for w in range(width):
                col = (xi * width + w) * LANES
                for pi in range(np_):
                    for zi in range(nz):
                        for s in range(ns):
                            row = pi * rows_p + (zi * ns + s) * rs
                            part[(g * width + w) * ns + s, pi, xi, zi] = grad[row:row + rs, col:col + LANES]

    per = width * ns
    stages = [stage_first, stage_second, stage_third, stage_own, stage_near, stage_relay, stage_far, stage_pre]
    lags = (-AHEAD,) + LAGS
    events = []
    for k in range(chunks):
        if kind(k) == "C":
            j = cs.index(k)
            slots = [CSLOTS[0]] + [slot + CSTEP * j for slot in CSLOTS[1:]]
        else:
            j = sum(kind(i) == kind(k) for i in range(k)) * (SA if kind(k) == "A" else SB) + (0 if kind(k) == "A" else OB)
            slots = [RATE * j - AHEAD] + [j + lag for lag in lags[1:]]
        events += [(slot, -i, k) for i, slot in enumerate(slots)]
    events.sort()
    done = 0
    waited = False
    for _, i, k in events:
        while done < groups and (done <= k // per or -i not in (0, 7)):
            compute(done)
            done += 1
        if not waited:
            pl.semaphore_wait(barrier, len(peers))
            waited = True
        stages[-i](k)
    drain()


def solution(mesh):
    np_, ndp = mesh.shape["pair"], mesh.shape["dp"]
    nx = 1
    while (2 * nx) ** 2 <= ndp and ndp % (2 * nx) == 0:
        nx *= 2
    nz = ndp // nx

    def local(activations, cotangents):
        rows, cols = activations.shape[1], cotangents.shape[1]
        nc = cols // nx // LANES
        ns = SPLIT
        width = 2 if nc % 2 == 0 else 1
        rs = rows // np_ // nz // ns
        chunks = nc * ns
        wide = max(np_, nx)
        half = max(1, nz // 2)
        cs = max(1, sum(KINDS[k % len(KINDS)] == "C" for k in range(chunks)))
        f32, bf16 = jnp.float32, jnp.bfloat16
        dma = pltpu.SemaphoreType.DMA
        activations, cotangents = (pltpu.with_memory_space_constraint(a, pltpu.HBM) for a in (activations, cotangents))
        return pl.pallas_call(
            functools.partial(kernel, np_, nx, nz, nc, ns),
            out_shape=jax.ShapeDtypeStruct((rows // np_, cols), jnp.bfloat16),
            in_specs=[pl.BlockSpec(memory_space=pltpu.HBM)] * 2,
            out_specs=pl.BlockSpec(memory_space=pltpu.VMEM),
            scratch_shapes=[
                pltpu.VMEM(activations.shape, activations.dtype),
                pltpu.VMEM((nc // width, cotangents.shape[0], nx * width * LANES), cotangents.dtype),
                pltpu.VMEM((rows, activations.shape[0]), activations.dtype),
                pltpu.VMEM((chunks, np_, nx, nz, rs, LANES), f32),
                pltpu.VMEM((chunks, np_, nx, nz, rs, LANES), bf16),
                pltpu.VMEM((chunks, np_ * nx, nz, rs, LANES), bf16),
                pltpu.VMEM((chunks, wide, nz, rs, LANES), bf16),
                pltpu.VMEM((chunks, nz, rs, LANES), bf16),
                pltpu.VMEM((cs, nz, np_, nx, rs, LANES), bf16),
                pltpu.VMEM((cs, half, half, np_, nx, rs, LANES), bf16),
                pltpu.VMEM((cs, np_, nx, rs, LANES), bf16),
                pltpu.VMEM((cs, nx, rs, LANES), bf16),
                dma((4,)), dma((chunks,)), dma((cs,)), dma((3,)), dma((chunks,)), dma((2,)), dma((chunks,)),
                dma((2,)), dma((2,)), dma((max(2, nz // 2),)), dma((chunks,)), dma((chunks,)), dma((3,)),
                dma((1 + nc // width * nx,)),
            ],
            compiler_params=pltpu.CompilerParams(
                collective_id=0, has_side_effects=True, vmem_limit_bytes=VM * 1024 * 1024),
        )(activations, cotangents)

    in_specs = (P(("pair", "dp"), "ep"), P(("pair", "dp"), "ep"))
    return jax.shard_map(local, mesh=mesh, in_specs=in_specs, out_specs=P("pair", "ep"), check_vma=False)
```

```python
import functools
import math

import jax
import jax.numpy as jnp
from jax import lax
from jax.experimental import pallas as pl
from jax.experimental.pallas import tpu as pltpu
from jax.sharding import PartitionSpec as P

LANES = 128
SPLIT = 2
POWER = 11
LARGEST_PRODUCT = 16 * 1.75
VM = 20
KINDS = "CCCABABABABABABA"
CSLOTS = (-9, 6, 11, 15, 19, 20, 24, 2)
CSTEP = 2
RATE = 1
SA = 2
SB = 2
OB = 1
DIRECT = 3
AHEAD = 5
LAGS = (0, 4, 9, 12, 13, 18)


def scale_and_offset(terms):
    scale = 2.0 ** math.floor(126 / POWER - math.log2(terms * LARGEST_PRODUCT))
    return scale, 2.0 ** (-124 / POWER)


def encode(x, terms):
    scale, offset = scale_and_offset(terms)
    a = x * scale + jnp.where(x < 0, -offset, offset)
    a2 = a * a
    a4 = a2 * a2
    return (a4 * a4 * (a2 * a)).astype(jnp.bfloat16)


def decode(f, terms):
    scale, offset = scale_and_offset(terms)
    f = f.astype(jnp.float32)
    a = jnp.exp2(jnp.log2(jnp.abs(f)) * (1 / POWER) - math.log2(scale)) - offset / scale
    return jnp.where(f < 0, -a, a)


def kernel(np_, nx, nz, nc, ns, act_hbm, cot_hbm, out_ref, act_ref, cot_ref, act_t, part, enc, f1, f2, zr, fc, fg, fy, fx,
           s1, r1, rg, s2, r2, sz, rz, sgz, sgx, sr, rn, rf, rl, load):
    p = lax.axis_index("pair")
    dp = lax.axis_index("dp")
    z, x = dp // nx, dp % nx
    rs = part.shape[-2]
    chunks = nc * ns
    rows_p = nz * ns * rs
    cols_x = nc * LANES
    terms = act_ref.shape[0]
    replicas = np_ * nx * nz
    half = max(1, nz // 2)
    low = z < half
    base = jnp.where(low, 0, half)
    far = jnp.where(low, half, 0)
    gateway = jnp.where(low, half - 1, half)
    opposite = jnp.where(low, half, half - 1)

    def other(i, q, n):
        return lax.rem(i + q, n)

    def to_pair(q):
        return {"pair": other(p, q, np_)}

    def to_x(q):
        return {"dp": z * nx + other(x, q, nx)}

    def at_z(zi):
        return {"dp": zi * nx + x}

    def near(q):
        return base + other(z - base, q, half)

    def kind(k):
        return KINDS[k % len(KINDS)]

    def direct(k):
        return k >= chunks - DIRECT

    def remote(src, dst, ssem, rsem, peer):
        return pltpu.make_async_remote_copy(
            src_ref=src, dst_ref=dst, send_sem=ssem, recv_sem=rsem,
            device_id=peer, device_id_type=pl.DeviceIdType.MESH)

    def arrived(ref, rsem):
        remote(ref, ref, rsem, rsem, to_pair(1)).wait_recv()

    def sent(ref, ssem):
        remote(ref, ref, ssem, ssem, to_pair(1)).wait_send()

    def piece(k, zi, xi):
        c, s = k // ns, k % ns
        row = pl.multiple_of((zi * ns + s) * rs, rs)
        col = pl.multiple_of(xi * cols_x + c * LANES, LANES)
        return out_ref.at[pl.ds(row, rs), pl.ds(col, LANES)]

    def spread(k, zi, xi, peer, ssem, rsem):
        here = piece(k, zi, xi)
        remote(here, here, ssem, rsem, peer).start()

    def gather_z(k):
        if nz > 1:
            spread(k, z, x, at_z(opposite), sgz.at[0], rf.at[k])
        for q in range(1, half):
            spread(k, z, x, at_z(near(q)), sgz.at[0], rn.at[k])

    def gather_x(k, zi):
        for q in range(1, nx):
            spread(k, zi, x, to_x(q), sgx.at[0], rl.at[0])

    def gather_all(k):
        for zo in range(nz):
            for q in range(nx):
                peer = {"dp": other(z, zo, nz) * nx + other(x, q, nx)}
                if q:
                    spread(k, z, x, peer, sgx.at[1], rl.at[1])
                elif zo:
                    spread(k, z, x, peer, sgz.at[1], rl.at[2])

    cs = [k for k in range(chunks) if kind(k) == "C"]

    def stage_first(k):
        if kind(k) == "C":
            c = cs.index(k)
            if half > 1:
                @pl.when(z != gateway)
                def _():
                    for j in range(half):
                        enc[k, :, :, far + j] = encode(part[k, :, :, far + j], terms)
                        remote(enc.at[k, :, :, far + j], fg.at[c, z - base, j], s1.at[3], rg.at[c], at_z(gateway)).start()
            for q in range(1, half):
                o = near(q)
                enc[k, :, :, o] = encode(part[k, :, :, o], terms)
                remote(enc.at[k, :, :, o], fc.at[c, z], s1.at[2], r1.at[k], at_z(o)).start()
        elif kind(k) == "A":
            for q in range(1, np_):
                o = other(p, q, np_)
                enc[k, o] = encode(part[k, o], terms)
                remote(enc.at[k, o], f1.at[k, pl.ds(p * nx, nx)], s1.at[0], r1.at[k], to_pair(q)).start()
        else:
            for q in range(1, nx):
                o = other(x, q, nx)
                enc[k, :, o] = encode(part[k, :, o], terms)
                remote(enc.at[k, :, o], f1.at[k, pl.ds(x * np_, np_)], s1.at[1], r1.at[k], to_x(q)).start()

    def stage_pre(k):
        c = cs.index(k)

        @pl.when(z == gateway)
        def _():
            if half > 1:
                arrived(fg.at[c, pl.ds(0, half - 1)], rg.at[c])
            for j in range(half):
                total = part[k, :, :, far + j]
                for q in range(1, half):
                    total = total + decode(fg[c, near(q) - base, j], terms)
                enc[k, :, :, far + j] = encode(total, half * terms)
                remote(enc.at[k, :, :, far + j], fc.at[c, base], s1.at[3], r1.at[k], at_z(far + j)).start()

    def stage_second(k):
        if kind(k) == "C":
            c = cs.index(k)
            arrived(fc.at[c, pl.ds(0, half)], r1.at[k])
            part[k, :, :, z] += decode(fc[c, far], half * terms)
            for q in range(1, half):
                part[k, :, :, z] += decode(fc[c, near(q)], terms)
            for q in range(1, np_):
                o = other(p, q, np_)
                enc[k, o, :, z] = encode(part[k, o, :, z], nz * terms)
                remote(enc.at[k, o, :, z], fy.at[cs.index(k), p], s2.at[2], r2.at[k], to_pair(q)).start()
        elif kind(k) == "A":
            arrived(f1.at[k, pl.ds(0, (np_ - 1) * nx)], r1.at[k])
            for q in range(1, np_):
                o = other(p, q, np_)
                part[k, p] += decode(f1[k, pl.ds(o * nx, nx)], terms)
            for q in range(1, nx):
                o = other(x, q, nx)
                enc[k, p, o] = encode(part[k, p, o], np_ * terms)
                remote(enc.at[k, p, o], f2.at[k, x], s2.at[0], r2.at[k], to_x(q)).start()
        else:
            arrived(f1.at[k, pl.ds(0, (nx - 1) * np_)], r1.at[k])
            for q in range(1, nx):
                o = other(x, q, nx)
                part[k, :, x] += decode(f1[k, pl.ds(o * np_, np_)], terms)
            for q in range(1, np_):
                o = other(p, q, np_)
                enc[k, o, x] = encode(part[k, o, x], nx * terms)
                remote(enc.at[k, o, x], f2.at[k, p], s2.at[1], r2.at[k], to_pair(q)).start()

    def stage_third(k):
        if kind(k) == "C":
            arrived(fy.at[cs.index(k), pl.ds(0, np_ - 1)], r2.at[k])
            for q in range(1, np_):
                part[k, p, :, z] += decode(fy[cs.index(k), other(p, q, np_)], nz * terms)
            for q in range(1, nx):
                o = other(x, q, nx)
                enc[k, p, o, z] = encode(part[k, p, o, z], np_ * nz * terms)
                remote(enc.at[k, p, o, z], fx.at[cs.index(k), x], sz.at[1], rz.at[k], to_x(q)).start()
            return
        n, i, count = (nx, x, np_) if kind(k) == "A" else (np_, p, nx)
        arrived(f2.at[k, pl.ds(0, n - 1)], r2.at[k])
        for q in range(1, n):
            part[k, p, x] += decode(f2[k, other(i, q, n)], count * terms)
        for q in range(1, nz):
            o = other(z, q, nz)
            enc[k, p, x, o] = encode(part[k, p, x, o], np_ * nx * terms)
            remote(enc.at[k, p, x, o], zr.at[k, z], sz.at[0], rz.at[k], at_z(o)).start()

    def stage_own(k):
        total = part[k, p, x, z]
        if kind(k) == "C":
            arrived(fx.at[cs.index(k), pl.ds(0, nx - 1)], rz.at[k])
            for q in range(1, nx):
                total = total + decode(fx[cs.index(k), other(x, q, nx)], np_ * nz * terms)
        elif nz > 1:
            arrived(zr.at[k, pl.ds(0, nz - 1)], rz.at[k])
        for q in range(1, nz if kind(k) != "C" else 1):
            total = total + decode(zr[k, other(z, q, nz)], np_ * nx * terms)
        piece(k, z, x)[...] = (total / replicas).astype(out_ref.dtype)
        if direct(k):
            gather_all(k)
        else:
            gather_z(k)
            gather_x(k, z)

    def stage_near(k):
        if half > 1 and not direct(k):
            arrived(enc.at[k, 0, 0, pl.ds(0, half - 1)], rn.at[k])
            for q in range(1, half):
                gather_x(k, near(q))

    def stage_relay(k):
        if half > 1 and not direct(k):
            @pl.when(z == gateway)
            def _():
                arrived(enc.at[k, 0, 0, pl.ds(0, half)], rf.at[k])
                for j in range(half):
                    for q in range(1, half):
                        spread(k, far + j, x, at_z(near(q)), sr.at[q], rf.at[k])

    def stage_far(k):
        if nz == 1 or direct(k):
            return
        if half > 1:
            @pl.when(z != gateway)
            def _():
                arrived(enc.at[k, 0, 0, pl.ds(0, half)], rf.at[k])
        else:
            arrived(enc.at[k, 0, 0, pl.ds(0, half)], rf.at[k])
        for j in range(half):
            gather_x(k, far + j)

    def drain():
        a, b, c = (sum(kind(k) == t for k in range(chunks)) for t in "ABC")
        g1 = sum(direct(k) for k in range(chunks))
        g0 = chunks - g1
        if a:
            sent(enc.at[pl.ds(0, a), pl.ds(0, np_ - 1)], s1.at[0])
            sent(enc.at[pl.ds(0, a), 0, pl.ds(0, nx - 1)], s2.at[0])
        if b:
            sent(enc.at[pl.ds(0, b), :, pl.ds(0, nx - 1)], s1.at[1])
            sent(enc.at[pl.ds(0, b), pl.ds(0, np_ - 1), 0], s2.at[1])
        if c:
            if half > 1:
                sent(enc.at[pl.ds(0, c), :, :, pl.ds(0, half - 1)], s1.at[2])
            sent(enc.at[pl.ds(0, c), :, :, pl.ds(0, half)], s1.at[3])
            sent(enc.at[pl.ds(0, c), pl.ds(0, np_ - 1), :, 0], s2.at[2])
            sent(enc.at[pl.ds(0, c), 0, pl.ds(0, nx - 1), 0], sz.at[1])
        if nz > 1 and a + b:
            sent(enc.at[pl.ds(0, a + b), 0, 0, pl.ds(0, nz - 1)], sz.at[0])
        if g0:
            if nz > 1:
                group = enc.at[pl.ds(0, g0), 0, 0, pl.ds(0, half)]
                sent(group, sgz.at[0])
                if half > 1:
                    @pl.when(z == gateway)
                    def _():
                        for q in range(1, half):
                            sent(group, sr.at[q])
            if nx > 1:
                sent(enc.at[pl.ds(0, g0), 0, pl.ds(0, nx - 1)], sgx.at[0])
                arrived(enc.at[pl.ds(0, g0), 0, pl.ds(0, nx - 1)], rl.at[0])
        if g1:
            if nz > 1:
                sent(enc.at[pl.ds(0, g1), 0, 0, pl.ds(0, nz - 1)], sgz.at[1])
                arrived(enc.at[pl.ds(0, g1), 0, 0, pl.ds(0, nz - 1)], rl.at[2])
            if nx > 1:
                sent(enc.at[pl.ds(0, g1), 0, pl.ds(0, nx - 1)], sgx.at[1])
                arrived(enc.at[pl.ds(0, g1), 0, pl.ds(0, nx - 1)], rl.at[1])

    width = 2 if nc % 2 == 0 else 1
    groups = nc // width
    blocks = [(g, xi) for g in range(groups) for xi in range(nx)]

    def block(g, xi):
        return pl.ds(xi * cols_x + g * (width * LANES), width * LANES)

    def held(xi):
        return pl.ds(xi * (width * LANES), width * LANES)

    loads = [pltpu.make_async_copy(act_hbm, act_ref, load.at[len(blocks)])]
    loads += [pltpu.make_async_copy(cot_hbm.at[:, block(g, xi)], cot_ref.at[g, :, held(xi)], load.at[i])
              for i, (g, xi) in enumerate(blocks)]
    for copy in loads:
        copy.start()

    barrier = pltpu.get_barrier_semaphore()
    peers = [to_pair(q) for q in range(1, np_)] + [{"dp": other(dp, q, nz * nx)} for q in range(1, nz * nx)]
    for peer in peers:
        pl.semaphore_signal(barrier, inc=1, device_id=peer, device_id_type=pl.DeviceIdType.MESH)

    loads[0].wait()
    act_t[...] = act_ref[...].T

    def compute(g):
        for xi in range(nx):
            loads[1 + g * nx + xi].wait()
        grad = jnp.dot(act_t[...], cot_ref[g], preferred_element_type=jnp.float32)
        for xi in range(nx):
            for w in range(width):
                col = (xi * width + w) * LANES
                for pi in range(np_):
                    for zi in range(nz):
                        for s in range(ns):
                            row = pi * rows_p + (zi * ns + s) * rs
                            part[(g * width + w) * ns + s, pi, xi, zi] = grad[row:row + rs, col:col + LANES]

    per = width * ns
    stages = [stage_first, stage_second, stage_third, stage_own, stage_near, stage_relay, stage_far, stage_pre]
    lags = (-AHEAD,) + LAGS
    events = []
    for k in range(chunks):
        if kind(k) == "C":
            j = cs.index(k)
            slots = [CSLOTS[0]] + [slot + CSTEP * j for slot in CSLOTS[1:]]
        else:
            j = sum(kind(i) == kind(k) for i in range(k)) * (SA if kind(k) == "A" else SB) + (0 if kind(k) == "A" else OB)
            slots = [RATE * j - AHEAD] + [j + lag for lag in lags[1:]]
        events += [(slot, -i, k) for i, slot in enumerate(slots)]
    events.sort()
    done = 0
    waited = False
    for _, i, k in events:
        while done < groups and (done <= k // per or -i not in (0, 7)):
            compute(done)
            done += 1
        if not waited:
            pl.semaphore_wait(barrier, len(peers))
            waited = True
        stages[-i](k)
    drain()


def solution(mesh):
    np_, ndp = mesh.shape["pair"], mesh.shape["dp"]
    nx = 1
    while (2 * nx) ** 2 <= ndp and ndp % (2 * nx) == 0:
        nx *= 2
    nz = ndp // nx

    def local(activations, cotangents):
        rows, cols = activations.shape[1], cotangents.shape[1]
        nc = cols // nx // LANES
        ns = SPLIT
        width = 2 if nc % 2 == 0 else 1
        rs = rows // np_ // nz // ns
        chunks = nc * ns
        wide = max(np_, nx)
        half = max(1, nz // 2)
        cs = max(1, sum(KINDS[k % len(KINDS)] == "C" for k in range(chunks)))
        f32, bf16 = jnp.float32, jnp.bfloat16
        dma = pltpu.SemaphoreType.DMA
        activations, cotangents = (pltpu.with_memory_space_constraint(a, pltpu.HBM) for a in (activations, cotangents))
        return pl.pallas_call(
            functools.partial(kernel, np_, nx, nz, nc, ns),
            out_shape=jax.ShapeDtypeStruct((rows // np_, cols), jnp.bfloat16),
            in_specs=[pl.BlockSpec(memory_space=pltpu.HBM)] * 2,
            out_specs=pl.BlockSpec(memory_space=pltpu.VMEM),
            scratch_shapes=[
                pltpu.VMEM(activations.shape, activations.dtype),
                pltpu.VMEM((nc // width, cotangents.shape[0], nx * width * LANES), cotangents.dtype),
                pltpu.VMEM((rows, activations.shape[0]), activations.dtype),
                pltpu.VMEM((chunks, np_, nx, nz, rs, LANES), f32),
                pltpu.VMEM((chunks, np_, nx, nz, rs, LANES), bf16),
                pltpu.VMEM((chunks, np_ * nx, nz, rs, LANES), bf16),
                pltpu.VMEM((chunks, wide, nz, rs, LANES), bf16),
                pltpu.VMEM((chunks, nz, rs, LANES), bf16),
                pltpu.VMEM((cs, nz, np_, nx, rs, LANES), bf16),
                pltpu.VMEM((cs, half, half, np_, nx, rs, LANES), bf16),
                pltpu.VMEM((cs, np_, nx, rs, LANES), bf16),
                pltpu.VMEM((cs, nx, rs, LANES), bf16),
                dma((4,)), dma((chunks,)), dma((cs,)), dma((3,)), dma((chunks,)), dma((2,)), dma((chunks,)),
                dma((2,)), dma((2,)), dma((max(2, nz // 2),)), dma((max(1, chunks - DIRECT),)), dma((max(1, chunks - DIRECT),)), dma((3,)),
                dma((1 + nc // width * nx,)),
            ],
            compiler_params=pltpu.CompilerParams(
                collective_id=0, has_side_effects=True, vmem_limit_bytes=VM * 1024 * 1024),
        )(activations, cotangents)

    in_specs = (P(("pair", "dp"), "ep"), P(("pair", "dp"), "ep"))
    return jax.shard_map(local, mesh=mesh, in_specs=in_specs, out_specs=P("pair", "ep"), check_vma=False)
```
